32 devices in a mesh: slab: 4 (over z), pencil: 8 (over y, x, core).
Axes of the slice: x: 2, y: 2, z: 4, core: 2. Of those that a mesh axis runs over, the one named last changes fastest.
Arguments:
- right_sides: float32 [8, 128, 128, 128], P(None, 'slab', 'pencil'), may hold values from -6 to 6
- spectrum: float32 [128, 128, 128], P('pencil', 'slab'), may hold values from 0.5 to 20, as said below
- noise_var: float32 [128, 128, 128], P('slab', 'pencil'), may hold values from 0.05 to 1
- observed: int32 [128, 128, 128], P('slab', 'pencil'), may hold values 0 or 1
Outputs:
- solution: float32 [8, 128, 128, 128], P(None, 'slab', 'pencil')
- noise_grad: float32 [128, 128, 128], P('slab', 'pencil')
The draws below stay inside these ranges and needn't reach their ends.
Inputs may be any that keep to these rules, and one draw needn't show every extreme that they name: Even in every index: spectrum[a, b, c] equals spectrum[(-a) mod 128, (-b) mod 128, (-c) mod 128].
All inputs are finite; a program needn't handle non-finite values. No bound on the sum of `observed` on one device may be relied on, other than what follows from the above.
Results may differ from the reference program's by a relative error of at most 0.00021.
Values sent between devices are 32-bit elements; how exact they have to be, the bound alone decides.
A program may use at most 128 MiB of HBM per device.

```python
import math
import jax
import jax.numpy as jnp
from jax import lax

NZ = 128
NY = 128
NX = 128
PROBES = 8
ITERS = 3


def draw_spectrum(key, part):
    base_values = jnp.exp(jax.random.uniform(key, (NX, NY, NZ), jnp.float32, math.log(0.5), math.log(20.0)))
    mirror = jnp.roll(jnp.flip(base_values, (0, 1, 2)), 1, (0, 1, 2))
    return 0.5 * (base_values + mirror)


def touch_ends(array, own_key, low, largest):
    extent = array.shape
    place = [jax.random.randint(jax.random.fold_in(own_key, axis), (), 0, extent[axis]) for axis in range(len(extent))]
    array = array.at[tuple(place)].set(low)
    longest = extent.index(max(extent))
    place[longest] = (place[longest] + 1) % extent[longest]
    return array.at[tuple(place)].set(largest)


def steps_of(own_key, extent, split, low, top_value):
    def one(position, parts):
        draws = jax.random.uniform(jax.random.fold_in(jax.random.fold_in(own_key, 6), position), (parts,), jnp.float32, low / len(split), top_value / len(split))
        return jnp.repeat(jnp.exp(draws), extent[position] // parts).reshape((-1,) + (1,) * (len(extent) - position - 1))

    factor_of = one(*split[0])
    for cut in split[1:]:
        factor_of = factor_of * one(*cut)
    return factor_of


def centred(rng, shape, deviation, reach, split=(), kind=jnp.bfloat16):
    factor_of = steps_of(rng, shape, split, -0.22, 0.18) if split else 1.0
    values = jax.random.normal(rng, shape, jnp.float32) * deviation * factor_of
    return jnp.minimum(jnp.maximum(values, -reach), reach).astype(kind)


def setup_inputs(seed: int = 0) -> dict:
    key_list = jax.random.split(jax.random.key(seed), 5)
    right_sides = centred(key_list[0], (PROBES, NZ, NY, NX), 1.0, 6.0, ((1, 4), (2, 8)), jnp.float32)
    spectrum = draw_spectrum(jax.random.fold_in(key_list[4], 71), 0)
    noise_var = jnp.clip(jnp.exp(math.log(1.0) - 2.9957323 * jax.random.uniform(key_list[2], (NZ, NY, NX), jnp.float32) ** steps_of(key_list[2], (NZ, NY, NX), ((0, 4), (1, 8)), -0.2, 0.2)), 0.05, 1.0)
    observed = touch_ends((jax.random.randint(key_list[3], (NZ, NY, NX), 0, 4) < 3).astype(jnp.int32), jax.random.fold_in(key_list[3], 1), 0, 1)
    return dict(right_sides=right_sides, spectrum=spectrum, noise_var=noise_var, observed=observed)


precise = lax.Precision.HIGHEST

def symmetric(matrix):
    return 0.5 * (matrix + matrix.T)

def solve_spd(matrix, right_hand):
    factor = jnp.linalg.cholesky(symmetric(matrix))
    halfway = lax.linalg.triangular_solve(factor, right_hand, left_side=True, lower=True)
    return lax.linalg.triangular_solve(factor, halfway, left_side=True, lower=True, transpose_a=True)

def gram_local(left, right):
    column_count = left.shape[0]
    return jnp.dot(left.reshape(column_count, -1), right.reshape(column_count, -1).T, precision=precise)

def combine(field_block, coefficients):
    column_count = field_block.shape[0]
    mixed = jnp.dot(coefficients.T, field_block.reshape(column_count, -1), precision=precise)
    return mixed.reshape(field_block.shape)

def operate(field_block, eigen_block, seen_cells, noise_var):
    masked = field_block * seen_cells
    spectral = jnp.fft.fftn(masked, axes=(1, 2, 3))
    smooth = jnp.real(jnp.fft.ifftn(spectral * eigen_block, axes=(1, 2, 3))).astype(jnp.float32)
    return seen_cells * smooth + noise_var * field_block

def reference(right_sides, spectrum, noise_var, observed):
    eigen_block = jnp.transpose(spectrum, (2, 1, 0))
    seen_cells = observed.astype(jnp.float32)
    solution = jnp.zeros_like(right_sides)
    residual = right_sides
    direction = right_sides
    gamma_now = gram_local(residual, residual)
    for iteration in range(ITERS):
        image_block = operate(direction, eigen_block, seen_cells, noise_var)
        delta_now = gram_local(direction, image_block)
        alpha_step = solve_spd(delta_now, gamma_now)
        solution = solution + combine(direction, alpha_step)
        if iteration + 1 < ITERS:
            residual = residual - combine(image_block, alpha_step)
            gamma_next = gram_local(residual, residual)
            beta_step = solve_spd(gamma_now, gamma_next)
            direction = residual + combine(direction, beta_step)
            gamma_now = gamma_next
    weights = right_sides[1:] * solution[1:]
    noise_grad = 0.5 * (solution[0] * solution[0] - jnp.mean(weights, axis=0))
    return (solution, noise_grad)
```

```python
import functools

import jax
import jax.numpy as jnp
import numpy as np
from jax import lax
from jax.experimental import pallas as pl
from jax.experimental.pallas import tpu as pltpu
from jax.sharding import PartitionSpec as P

ITERS = 3
SHIFT = 8.0
SCALE = 8.0
FLOOR = 3e-3
F32 = jnp.float32
BF16 = jnp.bfloat16
INTERPRET = False

precise = lax.Precision.HIGHEST


def embed(length, forward, scale=1.0):
    points = np.arange(length)
    angles = (points[:, None] * points[None, :] % length) * (2.0 * np.pi / length)
    cosine, sine = np.cos(angles) * scale, np.sin(angles) * scale
    if not forward:
        sine = -sine
    return np.block([[cosine, sine], [-sine, cosine]])


def halves(table):
    table = np.asarray(table, np.float32)
    high = table.astype(BF16)
    low = (table - high.astype(np.float32)).astype(BF16)
    return np.stack((high, low))


def split(values):
    high = values.astype(BF16)
    return high, (values - high.astype(F32)).astype(BF16)


def dot3(left, right, dims=((1,), (0,))):
    mul = functools.partial(
        lax.dot_general, dimension_numbers=(dims, ((), ())), preferred_element_type=F32
    )
    return mul(left[0], right[0]) + (mul(left[1], right[0]) + mul(left[0], right[1]))


def pair_of(ref):
    return ref[0], ref[1]


def forward_planes(planes, fx, fz):
    found = []
    for real, imag in planes:
        length = real.shape[1]
        first = dot3(fx, split(jnp.concatenate((real, imag), axis=1)), ((1,), (1,)))
        first = jnp.concatenate((first[:length], first[length:]), axis=1)
        found.append(dot3(split(first), fz))
    return jnp.swapaxes(jnp.stack(found), 0, 1)


def inverse_planes(values, gx, gz):
    rows = jnp.swapaxes(values, 0, 1)
    found = []
    for y in range(rows.shape[0]):
        first = dot3(split(rows[y]), gz)
        length = first.shape[1] // 2
        first = jnp.concatenate((first[:, :length], first[:, length:]), axis=0)
        plane = dot3(split(first), gx, ((0,), (0,)))
        width = plane.shape[1] // 2
        found.append((plane[:, :width], plane[:, width:]))
    return found


def planes_of(ref, y):
    count = ref.shape[0]
    return tuple(
        jnp.concatenate([ref[s, y, c] for s in range(count)], axis=0) for c in range(2)
    )


def lines_of(ref, y):
    return jnp.concatenate([ref[s, y] for s in range(ref.shape[0])], axis=0)


def first_kernel(w_ref, fx, fz, o_ref):
    planes = [planes_of(w_ref, y) for y in range(w_ref.shape[1])]
    o_ref[...] = forward_planes(planes, pair_of(fx), pair_of(fz))


def middle_kernel(d_ref, e_ref, fy, gy, o_ref):
    fy, gy = pair_of(fy), pair_of(gy)
    for a in range(d_ref.shape[1]):
        data = d_ref[:, a]
        data = data.reshape(-1, data.shape[-1])
        width = data.shape[1] // 2
        data = jnp.concatenate((data[:, :width], data[:, width:]), axis=0)
        spec = dot3(fy, split(data))
        eigen = e_ref[:, a].reshape(-1, e_ref.shape[-1])
        spec = spec * jnp.concatenate((eigen, eigen), axis=0)
        back = dot3(gy, split(spec))
        length = back.shape[0] // 2
        back = jnp.concatenate((back[:length], back[length:]), axis=1)
        o_ref[:, a] = back.reshape(o_ref.shape[0], o_ref.shape[2], o_ref.shape[3])


def next_kernel(u_ref, w_ref, n_ref, s_ref, gx, gz, fx, fz, w_out, o_ref):
    found = inverse_planes(u_ref[...], pair_of(gx), pair_of(gz))
    slabs, ys, _, depth, _ = w_ref.shape
    planes = []
    for y in range(ys):
        seen = lines_of(s_ref, y)
        noise = lines_of(n_ref, y) - SHIFT
        old = planes_of(w_ref, y)
        new = tuple((seen * t + noise * w) * (1.0 / SCALE) for t, w in zip(found[y], old))
        for s in range(slabs):
            for c in range(2):
                w_out[s, y, c] = new[c][s * depth : (s + 1) * depth]
        planes.append(new)
    o_ref[...] = forward_planes(planes, pair_of(fx), pair_of(fz))


def last_kernel(u_ref, gx, gz, w_out):
    found = inverse_planes(u_ref[...], pair_of(gx), pair_of(gz))
    slabs, ys, _, depth, _ = w_out.shape
    for y in range(ys):
        for s in range(slabs):
            for c in range(2):
                w_out[s, y, c] = found[y][c][s * depth : (s + 1) * depth]


def whole(shape):
    return pl.BlockSpec(shape, lambda i: (0,) * len(shape))


def along(shape, axis, block):
    full = tuple(block if d == axis else n for d, n in enumerate(shape))
    return pl.BlockSpec(full, lambda i: tuple(i if d == axis else 0 for d in range(len(shape))))


def call(kernel, args, specs, outs, out_specs, steps, flops=0):
    many = isinstance(outs, (list, tuple))
    return pl.pallas_call(
        kernel,
        grid=(steps,),
        in_specs=specs,
        out_specs=out_specs,
        out_shape=outs,
        interpret=INTERPRET,
        cost_estimate=pl.CostEstimate(
            flops=flops, bytes_accessed=sum(a.size * 4 for a in args), transcendentals=0
        ),
        compiler_params=pltpu.CompilerParams(vmem_limit_bytes=56 * 2**20),
    )(*args)


def gram_kernel(l_ref, r_ref, o_ref):
    quads, ys, both, depth, _ = l_ref.shape
    columns = quads * both
    tile = min(8, depth)
    index = [(i, j) for i in range(columns) for j in range(i, columns)]

    def load(ref, y, z):
        return [ref[i // both, y, i % both, pl.ds(z, tile)] for i in range(columns)]

    def body(step, sums):
        y = step // (depth // tile)
        z = pl.multiple_of(step % (depth // tile) * tile, tile)
        left, right = load(l_ref, y, z), load(r_ref, y, z)
        return tuple(s + left[i] * right[j] for s, (i, j) in zip(sums, index))

    zero = jnp.zeros((tile, l_ref.shape[-1]), F32)
    sums = lax.fori_loop(0, ys * (depth // tile), body, (zero,) * len(index))
    for total, (i, j) in zip(sums, index):
        row = jnp.sum(total, axis=0, keepdims=True)
        o_ref[pl.ds(i * columns + j, 1)] = row
        if i != j:
            o_ref[pl.ds(j * columns + i, 1)] = row


def moment(left, right):
    columns = left.shape[0] * left.shape[2]
    rows = pl.pallas_call(
        gram_kernel,
        out_shape=jax.ShapeDtypeStruct((columns * columns, left.shape[-1]), F32),
        interpret=INTERPRET,
        cost_estimate=pl.CostEstimate(
            flops=left.size * columns, bytes_accessed=left.size * 8, transcendentals=0
        ),
    )(left, right)
    return jnp.sum(rows, axis=1)


def solve(matrix, right_hand):
    size = matrix.shape[0]
    both = jnp.concatenate((0.5 * (matrix + matrix.T), right_hand), axis=1)
    place = lax.broadcasted_iota(jnp.int32, both.shape, 0)
    for i in range(size):
        row = both[i : i + 1] / both[i : i + 1, i : i + 1]
        both = jnp.where(place == i, row, both - both[:, i : i + 1] * row)
    return both[:, size:]


def least_pivots(matrix):
    size = matrix.shape[0]
    both = 0.5 * (matrix + matrix.T)
    place = lax.broadcasted_iota(jnp.int32, both.shape, 0)
    lane = lax.broadcasted_iota(jnp.int32, both.shape, 1)
    for i in range(size):
        row = both[i : i + 1] / both[i : i + 1, i : i + 1]
        both = jnp.where(place > i, both - both[:, i : i + 1] * row, both)
    return jnp.sum(jnp.where(place == lane, both, 0.0), axis=0, keepdims=True)


def dot(left, right):
    return jnp.dot(left, right, precision=precise, preferred_element_type=F32)


def small_kernel(h_ref, c_ref, ok_ref):
    hankel = h_ref[...]
    columns = hankel.shape[0] // (ITERS + 1)

    def operator(c):
        zero = jnp.zeros((columns, columns), F32)
        return SHIFT * c + SCALE * jnp.concatenate((zero, c[: ITERS * columns]), axis=0)

    def inner(u, v):
        return dot(u.T, dot(hankel, v))

    shape = (hankel.shape[0], columns)
    same = lax.broadcasted_iota(jnp.int32, shape, 0) == lax.broadcasted_iota(jnp.int32, shape, 1)
    residual = jnp.where(same, 1.0, 0.0).astype(F32)
    direction, answer = residual, jnp.zeros(shape, F32)
    gamma = hankel[:columns, :columns]
    start = least_pivots(gamma)
    fine = jnp.ones((1, columns), F32)
    for iteration in range(ITERS):
        image = operator(direction)
        alpha = solve(inner(direction, image), gamma)
        answer = answer + dot(direction, alpha)
        if iteration + 1 < ITERS:
            residual = residual - dot(image, alpha)
            gamma_next = inner(residual, residual)
            fine = jnp.where(least_pivots(gamma_next) > FLOOR * start, fine, 0.0)
            beta = solve(gamma, gamma_next)
            direction = residual + dot(direction, beta)
            gamma = gamma_next
    c_ref[...] = answer
    ok_ref[...] = fine


def final_kernel(c_ref, p0, p1, p2, x_ref, g_ref):
    quads, ys, both, depth, _ = p0.shape
    columns = quads * both
    tile = min(8, depth)
    basis = (p0, p1, p2)
    for half in range(2):
        span = range(half * columns // 2, (half + 1) * columns // 2)
        mix = [[c_ref[k * columns + i, p] for p in span] for k in range(3) for i in range(columns)]

        def body(step, carry):
            y = step // (depth // tile)
            rows = pl.ds(pl.multiple_of(step % (depth // tile) * tile, tile), tile)
            sums = [0.0] * len(span)
            for k in range(3):
                for i in range(columns):
                    value = basis[k][i // both, y, i % both, rows]
                    sums = [s + value * m for s, m in zip(sums, mix[k * columns + i])]
            grad = 0.0
            for s, p in zip(sums, span):
                x_ref[p // both, y, p % both, rows] = s
                if p == 0:
                    grad = grad + 0.5 * s * s
                else:
                    grad = grad - p0[p // both, y, p % both, rows] * s * (0.5 / (columns - 1))
            g_ref[y, rows] = grad if half == 0 else g_ref[y, rows] + grad
            return carry

        lax.fori_loop(0, ys * (depth // tile), body, 0)


def exchange(values, axis):
    return lax.all_to_all(values, axis, split_axis=0, concat_axis=0, tiled=True)


def recurrences(p0, p1, p2, u2):
    flat = lambda v: jnp.swapaxes(v, 1, 2).reshape(v.shape[0] * v.shape[2], -1)
    basis = [flat(v) for v in (p0, p1, p2, u2)]
    shape = (p0.shape[0], p0.shape[2], p0.shape[1]) + p0.shape[3:]
    columns = basis[0].shape[0]

    def field(c):
        return sum(dot(c[k].T, basis[k]) for k in range(len(c)))

    def gram(u, v):
        local_sum = jnp.dot(u, v.T, precision=precise)
        return lax.psum(local_sum, ("slab", "pencil"))

    def operator(c):
        zero = jnp.zeros((1, columns, columns), F32)
        return SHIFT * jnp.concatenate((c, zero)) + SCALE * jnp.concatenate((zero, c))

    def longer(c):
        return jnp.concatenate((c, jnp.zeros((1, columns, columns), F32)))

    residual = direction = answer = jnp.eye(columns, dtype=F32)[None]
    answer = 0.0 * answer
    vector = field(residual)
    gamma = gram(vector, vector)
    for iteration in range(ITERS):
        image = operator(direction)
        alpha = solve(gram(field(direction), field(image)), gamma)
        answer = answer + jnp.einsum("kij,jp->kip", direction, alpha, precision=precise)
        if iteration + 1 < ITERS:
            residual = longer(residual) - jnp.einsum("kij,jp->kip", image, alpha, precision=precise)
            vector = field(residual)
            gamma_next = gram(vector, vector)
            beta = solve(gamma, gamma_next)
            direction = residual + longer(
                jnp.einsum("kij,jp->kip", direction, beta, precision=precise)
            )
            answer = longer(answer)
            gamma = gamma_next
    return answer.reshape(-1, columns)


def local(right_sides, spectrum, noise_var, observed):
    columns, depth, ys, nx = right_sides.shape
    slabs, pencils = lax.axis_size("slab"), lax.axis_size("pencil")
    nz, ny = depth * slabs, ys * pencils
    seen = jnp.swapaxes(observed.astype(F32), 0, 1)
    noise = jnp.swapaxes(noise_var, 0, 1)
    field = jnp.transpose(right_sides.reshape(columns // 2, 2, depth, ys, nx), (0, 3, 1, 2, 4))

    own = columns // slabs
    quads = columns // 2

    def to_planes(values):
        if own % 2:
            values = jnp.swapaxes(values, 1, 2).reshape(columns, ys, 1, depth, nx)
            values = jnp.concatenate((values, jnp.zeros_like(values)), axis=2)
        return exchange(values, "slab")

    def from_planes(values):
        values = exchange(values, "slab")
        if own % 2:
            values = values[:, :, 0].reshape(quads, 2, ys, depth, nx)
            values = jnp.swapaxes(values, 1, 2)
        return values

    fx, gx = halves(embed(nx, True)), halves(embed(nx, False).T)
    fz, gz = halves(embed(nz, True).T), halves(embed(nz, False).T)
    fy, gy = halves(embed(ny, True)), halves(embed(ny, False, 1.0 / (nx * ny * nz)))
    fx, gx, fz, gz, fy, gy = (jnp.asarray(t) for t in (fx, gx, fz, gz, fy, gy))

    part = nx // pencils
    chunk = 8 if ys % 8 == 0 else ys
    wide = 2 * nz
    tables = lambda *ts: [whole(t.shape) for t in ts]
    sent_shape = (nx, ys, wide)
    work = 12 * 2 * ys * nx * nz * 2 * (nx + nz)

    w0 = to_planes(field * seen[None, :, None])
    shape = w0.shape
    w_spec = along(shape, 1, chunk)
    sent_spec = along(sent_shape, 1, chunk)
    steps = ys // chunk
    sent = call(
        first_kernel, (w0, fx, fz), [w_spec] + tables(fx, fz),
        jax.ShapeDtypeStruct(sent_shape, F32), sent_spec, steps, work,
    )
    eigen = lax.all_gather(spectrum, "slab")
    noise_all = lax.all_gather(noise, "slab")
    seen_all = lax.all_gather(seen, "slab")
    m_spec = along(noise_all.shape, 1, chunk)

    def middle(sent):
        got = exchange(sent.reshape(pencils, part, ys, wide), "pencil")
        if ys % 8:
            got = jnp.swapaxes(got, 0, 1).reshape(1, part, ny, wide)
        e = eigen
        if e.shape[2] % 8:
            e = jnp.swapaxes(e, 0, 1).reshape(1, part, ny, nz)
        block = min(4, part)
        back = call(
            middle_kernel, (got, e, fy, gy),
            [along(got.shape, 1, block), along(e.shape, 1, block)] + tables(fy, gy),
            jax.ShapeDtypeStruct(got.shape, F32), along(got.shape, 1, block), part // block, work,
        )
        if ys % 8:
            back = jnp.swapaxes(back.reshape(part, pencils, ys, wide), 0, 1)
        return exchange(back, "pencil").reshape(sent_shape)

    def advance(w, sent):
        return call(
            next_kernel, (middle(sent), w, noise_all, seen_all, gx, gz, fx, fz),
            [sent_spec, w_spec, m_spec, m_spec] + tables(gx, gz, fx, fz),
            (jax.ShapeDtypeStruct(shape, F32), jax.ShapeDtypeStruct(sent_shape, F32)),
            (w_spec, sent_spec), steps, 2 * work,
        )

    w1, sent = advance(w0, sent)
    w2, sent = advance(w1, sent)
    t3 = call(
        last_kernel, (middle(sent), gx, gz), [sent_spec] + tables(gx, gz),
        jax.ShapeDtypeStruct(shape, F32), w_spec, steps, work,
    )

    seen_here, factor = seen[None, :, None], ((noise - SHIFT) * (1.0 / SCALE))[None, :, None]
    p0 = field
    p1 = jnp.where(seen_here > 0, from_planes(w1), factor * p0)
    p2 = jnp.where(seen_here > 0, from_planes(w2), factor * (factor * p0))
    u2 = (1.0 / SCALE) * seen_here * from_planes(t3) + factor * p2
    sums = [moment(l, r) for l, r in ((p0, p0), (p0, p1), (p1, p1), (p1, p2), (p2, p2), (p2, u2))]
    sums = lax.psum(jnp.stack(sums), ("slab", "pencil"))
    sums = [s.reshape(columns, columns) for s in sums] + [jnp.zeros((columns, columns), F32)]
    hankel = jnp.concatenate(
        [jnp.concatenate([sums[min(j + k, 6)] for k in range(4)], axis=1) for j in range(4)], axis=0
    )
    coefficients, fine = pl.pallas_call(
        small_kernel,
        out_shape=(
            jax.ShapeDtypeStruct((4 * columns, columns), F32),
            jax.ShapeDtypeStruct((1, columns), F32),
        ),
        interpret=INTERPRET,
    )(hankel)
    coefficients = lax.cond(
        jnp.min(fine) > 0.5,
        lambda: coefficients[: 3 * columns],
        lambda: recurrences(p0, p1, p2, u2),
    )
    answer, grad = pl.pallas_call(
        final_kernel,
        in_specs=[pl.BlockSpec(memory_space=pltpu.SMEM)]
        + [pl.BlockSpec(memory_space=pltpu.VMEM)] * 3,
        out_shape=(
            jax.ShapeDtypeStruct(field.shape, F32),
            jax.ShapeDtypeStruct((ys, depth, nx), F32),
        ),
        interpret=INTERPRET,
    )(coefficients, p0, p1, p2)
    answer = jnp.transpose(answer, (0, 2, 3, 1, 4)).reshape(columns, depth, ys, nx)
    return answer, jnp.swapaxes(grad, 0, 1)


def solution(mesh):
    in_specs = (
        P(None, "slab", "pencil", None),
        P("pencil", "slab", None),
        P("slab", "pencil", None),
        P("slab", "pencil", None),
    )
    out_specs = (P(None, "slab", "pencil", None), P("slab", "pencil", None))
    return jax.shard_map(local, mesh=mesh, in_specs=in_specs, out_specs=out_specs, check_vma=False)
```

```python
import functools

import jax
import jax.numpy as jnp
import numpy as np
from jax import lax
from jax.experimental import pallas as pl
from jax.experimental.pallas import tpu as pltpu
from jax.sharding import PartitionSpec as P

ITERS = 3
SHIFT = 8.0
SCALE = 8.0
FLOOR = 3e-3
F32 = jnp.float32
BF16 = jnp.bfloat16
INTERPRET = False

precise = lax.Precision.HIGHEST


def embed(length, forward, scale=1.0):
    points = np.arange(length)
    angles = (points[:, None] * points[None, :] % length) * (2.0 * np.pi / length)
    cosine, sine = np.cos(angles) * scale, np.sin(angles) * scale
    if not forward:
        sine = -sine
    return np.block([[cosine, sine], [-sine, cosine]])


def halves(table):
    table = np.asarray(table, np.float32)
    high = table.astype(BF16)
    low = (table - high.astype(np.float32)).astype(BF16)
    return np.stack((high, low))


def split(values):
    high = values.astype(BF16)
    return high, (values - high.astype(F32)).astype(BF16)


def dot3(left, right, dims=((1,), (0,))):
    mul = functools.partial(
        lax.dot_general, dimension_numbers=(dims, ((), ())), preferred_element_type=F32
    )
    return mul(left[0], right[0]) + (mul(left[1], right[0]) + mul(left[0], right[1]))


def pair_of(ref):
    return ref[0], ref[1]


def forward_planes(planes, fx, fz):
    found = []
    for real, imag in planes:
        length = real.shape[1]
        first = dot3(fx, split(jnp.concatenate((real, imag), axis=1)), ((1,), (1,)))
        first = jnp.concatenate((first[:length], first[length:]), axis=1)
        found.append(dot3(split(first), fz))
    return jnp.swapaxes(jnp.stack(found), 0, 1)


def inverse_planes(values, gx, gz):
    rows = jnp.swapaxes(values, 0, 1)
    found = []
    for y in range(rows.shape[0]):
        first = dot3(split(rows[y]), gz)
        length = first.shape[1] // 2
        first = jnp.concatenate((first[:, :length], first[:, length:]), axis=0)
        plane = dot3(split(first), gx, ((0,), (0,)))
        width = plane.shape[1] // 2
        found.append((plane[:, :width], plane[:, width:]))
    return found


def planes_of(ref, y):
    count = ref.shape[0]
    return tuple(
        jnp.concatenate([ref[s, y, c] for s in range(count)], axis=0) for c in range(2)
    )


def lines_of(ref, y):
    return jnp.concatenate([ref[s, y] for s in range(ref.shape[0])], axis=0)


def first_kernel(w_ref, fx, fz, o_ref):
    planes = [planes_of(w_ref, y) for y in range(w_ref.shape[1])]
    o_ref[...] = forward_planes(planes, pair_of(fx), pair_of(fz))


def middle_kernel(d_ref, e_ref, fy, gy, o_ref):
    fy, gy = pair_of(fy), pair_of(gy)
    for a in range(d_ref.shape[1]):
        data = d_ref[:, a]
        data = data.reshape(-1, data.shape[-1])
        width = data.shape[1] // 2
        data = jnp.concatenate((data[:, :width], data[:, width:]), axis=0)
        spec = dot3(fy, split(data))
        eigen = e_ref[:, a].reshape(-1, e_ref.shape[-1])
        spec = spec * jnp.concatenate((eigen, eigen), axis=0)
        back = dot3(gy, split(spec))
        length = back.shape[0] // 2
        back = jnp.concatenate((back[:length], back[length:]), axis=1)
        o_ref[:, a] = back.reshape(o_ref.shape[0], o_ref.shape[2], o_ref.shape[3])


def next_kernel(u_ref, w_ref, n_ref, s_ref, gx, gz, fx, fz, w_out, o_ref):
    found = inverse_planes(u_ref[...], pair_of(gx), pair_of(gz))
    slabs, ys, _, depth, _ = w_ref.shape
    planes = []
    for y in range(ys):
        seen = lines_of(s_ref, y)
        noise = lines_of(n_ref, y) - SHIFT
        old = planes_of(w_ref, y)
        new = tuple((seen * t + noise * w) * (1.0 / SCALE) for t, w in zip(found[y], old))
        for s in range(slabs):
            for c in range(2):
                w_out[s, y, c] = new[c][s * depth : (s + 1) * depth]
        planes.append(new)
    o_ref[...] = forward_planes(planes, pair_of(fx), pair_of(fz))


def last_kernel(u_ref, gx, gz, w_out):
    found = inverse_planes(u_ref[...], pair_of(gx), pair_of(gz))
    slabs, ys, _, depth, _ = w_out.shape
    for y in range(ys):
        for s in range(slabs):
            for c in range(2):
                w_out[s, y, c] = found[y][c][s * depth : (s + 1) * depth]


def whole(shape):
    return pl.BlockSpec(shape, lambda i: (0,) * len(shape))


def along(shape, axis, block):
    full = tuple(block if d == axis else n for d, n in enumerate(shape))
    return pl.BlockSpec(full, lambda i: tuple(i if d == axis else 0 for d in range(len(shape))))


def call(kernel, args, specs, outs, out_specs, steps, flops=0):
    many = isinstance(outs, (list, tuple))
    return pl.pallas_call(
        kernel,
        grid=(steps,),
        in_specs=specs,
        out_specs=out_specs,
        out_shape=outs,
        interpret=INTERPRET,
        cost_estimate=pl.CostEstimate(
            flops=flops, bytes_accessed=sum(a.size * 4 for a in args), transcendentals=0
        ),
        compiler_params=pltpu.CompilerParams(vmem_limit_bytes=56 * 2**20),
    )(*args)


def gram_kernel(l_ref, r_ref, o_ref):
    quads, ys, both, depth, _ = l_ref.shape
    columns = quads * both
    tile = min(8, depth)
    index = [(i, j) for i in range(columns) for j in range(i, columns)]

    def load(ref, y, z):
        return [ref[i // both, y, i % both, pl.ds(z, tile)] for i in range(columns)]

    def body(step, sums):
        y = step // (depth // tile)
        z = pl.multiple_of(step % (depth // tile) * tile, tile)
        left, right = load(l_ref, y, z), load(r_ref, y, z)
        return tuple(s + left[i] * right[j] for s, (i, j) in zip(sums, index))

    zero = jnp.zeros((tile, l_ref.shape[-1]), F32)
    sums = lax.fori_loop(0, ys * (depth // tile), body, (zero,) * len(index))
    for total, (i, j) in zip(sums, index):
        row = jnp.sum(total, axis=0, keepdims=True)
        o_ref[pl.ds(i * columns + j, 1)] = row
        if i != j:
            o_ref[pl.ds(j * columns + i, 1)] = row


def moment(left, right):
    columns = left.shape[0] * left.shape[2]
    rows = pl.pallas_call(
        gram_kernel,
        out_shape=jax.ShapeDtypeStruct((columns * columns, left.shape[-1]), F32),
        interpret=INTERPRET,
        cost_estimate=pl.CostEstimate(
            flops=left.size * columns, bytes_accessed=left.size * 8, transcendentals=0
        ),
    )(left, right)
    return jnp.sum(rows, axis=1)


def solve(matrix, right_hand):
    size = matrix.shape[0]
    both = jnp.concatenate((0.5 * (matrix + matrix.T), right_hand), axis=1)
    place = lax.broadcasted_iota(jnp.int32, both.shape, 0)
    for i in range(size):
        row = both[i : i + 1] / both[i : i + 1, i : i + 1]
        both = jnp.where(place == i, row, both - both[:, i : i + 1] * row)
    return both[:, size:]


def least_pivots(matrix):
    size = matrix.shape[0]
    both = 0.5 * (matrix + matrix.T)
    place = lax.broadcasted_iota(jnp.int32, both.shape, 0)
    lane = lax.broadcasted_iota(jnp.int32, both.shape, 1)
    for i in range(size):
        row = both[i : i + 1] / both[i : i + 1, i : i + 1]
        both = jnp.where(place > i, both - both[:, i : i + 1] * row, both)
    return jnp.sum(jnp.where(place == lane, both, 0.0), axis=0, keepdims=True)


def dot(left, right):
    return jnp.dot(left, right, precision=precise, preferred_element_type=F32)


def small_kernel(h_ref, c_ref, ok_ref):
    hankel = h_ref[...]
    columns = hankel.shape[0] // (ITERS + 1)

    def operator(c):
        zero = jnp.zeros((columns, columns), F32)
        return SHIFT * c + SCALE * jnp.concatenate((zero, c[: ITERS * columns]), axis=0)

    def inner(u, v):
        return dot(u.T, dot(hankel, v))

    shape = (hankel.shape[0], columns)
    same = lax.broadcasted_iota(jnp.int32, shape, 0) == lax.broadcasted_iota(jnp.int32, shape, 1)
    residual = jnp.where(same, 1.0, 0.0).astype(F32)
    direction, answer = residual, jnp.zeros(shape, F32)
    gamma = hankel[:columns, :columns]
    start = least_pivots(gamma)
    fine = jnp.ones((1, columns), F32)
    for iteration in range(ITERS):
        image = operator(direction)
        alpha = solve(inner(direction, image), gamma)
        answer = answer + dot(direction, alpha)
        if iteration + 1 < ITERS:
            residual = residual - dot(image, alpha)
            gamma_next = inner(residual, residual)
            fine = jnp.where(least_pivots(gamma_next) > FLOOR * start, fine, 0.0)
            beta = solve(gamma, gamma_next)
            direction = residual + dot(direction, beta)
            gamma = gamma_next
    c_ref[...] = answer
    ok_ref[...] = fine


def final_kernel(c_ref, p0, p1, p2, x_ref, g_ref):
    quads, ys, both, depth, _ = p0.shape
    columns = quads * both
    tile = min(8, depth)
    basis = (p0, p1, p2)
    for half in range(2):
        span = range(half * columns // 2, (half + 1) * columns // 2)
        mix = [[c_ref[k * columns + i, p] for p in span] for k in range(3) for i in range(columns)]

        def body(step, carry):
            y = step // (depth // tile)
            rows = pl.ds(pl.multiple_of(step % (depth // tile) * tile, tile), tile)
            sums = [0.0] * len(span)
            for k in range(3):
                for i in range(columns):
                    value = basis[k][i // both, y, i % both, rows]
                    sums = [s + value * m for s, m in zip(sums, mix[k * columns + i])]
            grad = 0.0
            for s, p in zip(sums, span):
                x_ref[p // both, y, p % both, rows] = s
                if p == 0:
                    grad = grad + 0.5 * s * s
                else:
                    grad = grad - p0[p // both, y, p % both, rows] * s * (0.5 / (columns - 1))
            g_ref[y, rows] = grad if half == 0 else g_ref[y, rows] + grad
            return carry

        lax.fori_loop(0, ys * (depth // tile), body, 0)


def travel_kernel(plan, sizes, *refs):
    count = len(plan)
    sources, targets = refs[:count], refs[count : 2 * count]
    send_sem, recv_sem, own_sem = refs[2 * count :]
    axes = tuple(dict.fromkeys(axis for axis, _ in plan))
    place = {axis: lax.axis_index(axis) for axis in sizes}
    barrier = pltpu.get_barrier_semaphore()

    def peer(axis, step):
        other = lax.rem(place[axis] + step, sizes[axis])
        return tuple(other if name == axis else place[name] for name in sizes)

    total = 0
    for axis in axes:
        for step in range(1, sizes[axis]):
            pl.semaphore_signal(
                barrier, inc=1, device_id=peer(axis, step), device_id_type=pl.DeviceIdType.MESH
            )
            total += 1
    pl.semaphore_wait(barrier, total)
    copies = []
    slot = 0
    order = []
    for number, (axis, gather) in enumerate(plan):
        for step in range(1, sizes[axis]):
            order.append((abs(2 * step - sizes[axis]), number, step, slot))
            slot += 1
    for _, number, step, slot in sorted(order):
        axis, gather = plan[number]
        other = lax.rem(place[axis] + step, sizes[axis])
        source = sources[number] if gather else sources[number].at[other]
        copy = pltpu.make_async_remote_copy(
            src_ref=source,
            dst_ref=targets[number].at[place[axis]],
            send_sem=send_sem.at[slot],
            recv_sem=recv_sem.at[slot],
            device_id=peer(axis, step),
            device_id_type=pl.DeviceIdType.MESH,
        )
        copy.start()
        copies.append(copy)
    for number, (axis, gather) in enumerate(plan):
        source = sources[number] if gather else sources[number].at[place[axis]]
        copy = pltpu.make_async_copy(
            source, targets[number].at[place[axis]], own_sem.at[number]
        )
        copy.start()
        copies.append(copy)
    for copy in copies:
        copy.wait()


def travel(identity, *moves):
    sizes = {name: lax.axis_size(name) for name in ("slab", "pencil")}
    plan = tuple((axis, gather) for _, axis, gather in moves)
    arrays = [array for array, _, _ in moves]
    slots = sum(sizes[axis] - 1 for axis, _ in plan)
    outs = tuple(
        jax.ShapeDtypeStruct(((sizes[axis],) if gather else ()) + array.shape, array.dtype)
        for array, axis, gather in moves
    )
    if INTERPRET:
        found = [
            lax.all_gather(v, axis) if gather else lax.all_to_all(v, axis, 0, 0, tiled=True)
            for v, axis, gather in moves
        ]
        return found
    return pl.pallas_call(
        functools.partial(travel_kernel, plan, sizes),
        in_specs=[pl.BlockSpec(memory_space=pltpu.VMEM)] * len(arrays),
        out_specs=(pl.BlockSpec(memory_space=pltpu.VMEM),) * len(arrays),
        out_shape=outs,
        scratch_shapes=[
            pltpu.SemaphoreType.DMA((slots,)),
            pltpu.SemaphoreType.DMA((slots,)),
            pltpu.SemaphoreType.DMA((len(arrays),)),
        ],
        cost_estimate=pl.CostEstimate(flops=0, bytes_accessed=2**26, transcendentals=0),
        compiler_params=pltpu.CompilerParams(collective_id=identity, has_side_effects=True),
    )(*arrays)


def recurrences(p0, p1, p2, u2):
    flat = lambda v: jnp.swapaxes(v, 1, 2).reshape(v.shape[0] * v.shape[2], -1)
    basis = [flat(v) for v in (p0, p1, p2, u2)]
    shape = (p0.shape[0], p0.shape[2], p0.shape[1]) + p0.shape[3:]
    columns = basis[0].shape[0]

    def field(c):
        return sum(dot(c[k].T, basis[k]) for k in range(len(c)))

    def gram(u, v):
        local_sum = jnp.dot(u, v.T, precision=precise)
        return lax.psum(local_sum, ("slab", "pencil"))

    def operator(c):
        zero = jnp.zeros((1, columns, columns), F32)
        return SHIFT * jnp.concatenate((c, zero)) + SCALE * jnp.concatenate((zero, c))

    def longer(c):
        return jnp.concatenate((c, jnp.zeros((1, columns, columns), F32)))

    residual = direction = answer = jnp.eye(columns, dtype=F32)[None]
    answer = 0.0 * answer
    vector = field(residual)
    gamma = gram(vector, vector)
    for iteration in range(ITERS):
        image = operator(direction)
        alpha = solve(gram(field(direction), field(image)), gamma)
        answer = answer + jnp.einsum("kij,jp->kip", direction, alpha, precision=precise)
        if iteration + 1 < ITERS:
            residual = longer(residual) - jnp.einsum("kij,jp->kip", image, alpha, precision=precise)
            vector = field(residual)
            gamma_next = gram(vector, vector)
            beta = solve(gamma, gamma_next)
            direction = residual + longer(
                jnp.einsum("kij,jp->kip", direction, beta, precision=precise)
            )
            answer = longer(answer)
            gamma = gamma_next
    return answer.reshape(-1, columns)


def local(right_sides, spectrum, noise_var, observed):
    columns, depth, ys, nx = right_sides.shape
    slabs, pencils = lax.axis_size("slab"), lax.axis_size("pencil")
    nz, ny = depth * slabs, ys * pencils
    seen = jnp.swapaxes(observed.astype(F32), 0, 1)
    noise = jnp.swapaxes(noise_var, 0, 1)
    field = jnp.transpose(right_sides.reshape(columns // 2, 2, depth, ys, nx), (0, 3, 1, 2, 4))

    own = columns // slabs
    quads = columns // 2

    def to_planes(values):
        if own % 2:
            values = jnp.swapaxes(values, 1, 2).reshape(columns, ys, 1, depth, nx)
            values = jnp.concatenate((values, jnp.zeros_like(values)), axis=2)
        return travel(0, (values, "slab", False))[0]

    def from_planes(values):
        if own % 2:
            values = values[:, :, 0].reshape(quads, 2, ys, depth, nx)
            values = jnp.swapaxes(values, 1, 2)
        return values

    fx, gx = halves(embed(nx, True)), halves(embed(nx, False).T)
    fz, gz = halves(embed(nz, True).T), halves(embed(nz, False).T)
    fy, gy = halves(embed(ny, True)), halves(embed(ny, False, 1.0 / (nx * ny * nz)))
    fx, gx, fz, gz, fy, gy = (jnp.asarray(t) for t in (fx, gx, fz, gz, fy, gy))

    part = nx // pencils
    chunk = 8 if ys % 8 == 0 else ys
    wide = 2 * nz
    tables = lambda *ts: [whole(t.shape) for t in ts]
    sent_shape = (nx, ys, wide)
    work = 12 * 2 * ys * nx * nz * 2 * (nx + nz)

    w0 = to_planes(field * seen[None, :, None])
    shape = w0.shape
    w_spec = along(shape, 1, chunk)
    sent_spec = along(sent_shape, 1, chunk)
    steps = ys // chunk
    sent = call(
        first_kernel, (w0, fx, fz), [w_spec] + tables(fx, fz),
        jax.ShapeDtypeStruct(sent_shape, F32), sent_spec, steps, work,
    )
    m_spec = along((slabs, ys, depth, nx), 1, chunk)

    def blocks(sent):
        return sent.reshape(pencils, part, ys, wide), "pencil", False

    def middle(got, eigen):
        if ys % 8:
            got = jnp.swapaxes(got, 0, 1).reshape(1, part, ny, wide)
        if eigen.shape[2] % 8:
            eigen = jnp.swapaxes(eigen, 0, 1).reshape(1, part, ny, nz)
        block = min(4, part)
        back = call(
            middle_kernel, (got, eigen, fy, gy),
            [along(got.shape, 1, block), along(eigen.shape, 1, block)] + tables(fy, gy),
            jax.ShapeDtypeStruct(got.shape, F32), along(got.shape, 1, block), part // block, work,
        )
        if ys % 8:
            back = jnp.swapaxes(back.reshape(part, pencils, ys, wide), 0, 1)
        return back, "pencil", False

    def advance(w, got):
        return call(
            next_kernel, (got.reshape(sent_shape), w, noise_all, seen_all, gx, gz, fx, fz),
            [sent_spec, w_spec, m_spec, m_spec] + tables(gx, gz, fx, fz),
            (jax.ShapeDtypeStruct(shape, F32), jax.ShapeDtypeStruct(sent_shape, F32)),
            (w_spec, sent_spec), steps, 2 * work,
        )

    got, eigen = travel(1, blocks(sent), (spectrum, "slab", True))
    got, noise_all, seen_all = travel(
        2, middle(got, eigen), (noise, "slab", True), (seen, "slab", True)
    )
    plane, sent = advance(w0, got)
    got, w1 = travel(3, blocks(sent), (plane, "slab", False))
    (got,) = travel(4, middle(got, eigen))
    w2, sent = advance(plane, got)
    got, w2 = travel(5, blocks(sent), (w2, "slab", False))
    (got,) = travel(6, middle(got, eigen))
    t3 = call(
        last_kernel, (got.reshape(sent_shape), gx, gz), [sent_spec] + tables(gx, gz),
        jax.ShapeDtypeStruct(shape, F32), w_spec, steps, work,
    )
    (t3,) = travel(7, (t3, "slab", False))

    seen_here, factor = seen[None, :, None], ((noise - SHIFT) * (1.0 / SCALE))[None, :, None]
    p0 = field
    p1 = jnp.where(seen_here > 0, from_planes(w1), factor * p0)
    p2 = jnp.where(seen_here > 0, from_planes(w2), factor * (factor * p0))
    u2 = (1.0 / SCALE) * seen_here * from_planes(t3) + factor * p2
    sums = [moment(l, r) for l, r in ((p0, p0), (p0, p1), (p1, p1), (p1, p2), (p2, p2), (p2, u2))]
    zeros = jnp.zeros((2, columns * columns), F32)
    (sums,) = travel(8, (jnp.concatenate((jnp.stack(sums), zeros)), "pencil", True))
    (sums,) = travel(9, (jnp.sum(sums, axis=0), "slab", True))
    sums = jnp.sum(sums, axis=0)[:6]
    sums = [s.reshape(columns, columns) for s in sums] + [jnp.zeros((columns, columns), F32)]
    hankel = jnp.concatenate(
        [jnp.concatenate([sums[min(j + k, 6)] for k in range(4)], axis=1) for j in range(4)], axis=0
    )
    coefficients, fine = pl.pallas_call(
        small_kernel,
        out_shape=(
            jax.ShapeDtypeStruct((4 * columns, columns), F32),
            jax.ShapeDtypeStruct((1, columns), F32),
        ),
        interpret=INTERPRET,
    )(hankel)
    coefficients = lax.cond(
        jnp.min(fine) > 0.5,
        lambda: coefficients[: 3 * columns],
        lambda: recurrences(p0, p1, p2, u2),
    )
    answer, grad = pl.pallas_call(
        final_kernel,
        in_specs=[pl.BlockSpec(memory_space=pltpu.SMEM)]
        + [pl.BlockSpec(memory_space=pltpu.VMEM)] * 3,
        out_shape=(
            jax.ShapeDtypeStruct(field.shape, F32),
            jax.ShapeDtypeStruct((ys, depth, nx), F32),
        ),
        interpret=INTERPRET,
    )(coefficients, p0, p1, p2)
    answer = jnp.transpose(answer, (0, 2, 3, 1, 4)).reshape(columns, depth, ys, nx)
    return answer, jnp.swapaxes(grad, 0, 1)


def solution(mesh):
    in_specs = (
        P(None, "slab", "pencil", None),
        P("pencil", "slab", None),
        P("slab", "pencil", None),
        P("slab", "pencil", None),
    )
    out_specs = (P(None, "slab", "pencil", None), P("slab", "pencil", None))
    return jax.shard_map(local, mesh=mesh, in_specs=in_specs, out_specs=out_specs, check_vma=False)
```
